1024 devices in a mesh: dp: 16 (over z), tensor: 8 (over y_lo, core), section: 8 (over x, y_hi).
Axes of the slice: x: 4, y: 8 (y_hi: 2, y_lo: 4; y = y_hi * 4 + y_lo), z: 16, core: 2. Of those that a mesh axis runs over, the one named last changes fastest.
Arguments:
- tokens: bfloat16 [1024, 8192], P('section', 'tensor'), may hold values from -6 to 6
- cotangent: bfloat16 [1024, 8192], P('section', 'tensor'), may hold values from -6 to 6
- gate_weight: bfloat16 [8192, 15360], P(('tensor', 'section'), 'dp'), may hold values from -0.0625 to 0.0625
- up_weight: bfloat16 [8192, 15360], P(('tensor', 'section'), 'dp'), may hold values from -0.0625 to 0.0625
- down_weight: bfloat16 [8192, 15360], P(('tensor', 'section'), 'dp'), may hold values from -0.046875 to 0.046875
Outputs:
- mixed: bfloat16 [1024, 8192], P(('section', 'dp'), 'tensor')
- input_grad: bfloat16 [1024, 8192], P(('section', 'dp'), 'tensor')
The draws below stay inside these ranges and needn't reach their ends.
All inputs are finite; a program needn't handle non-finite values.
Results may differ from the reference program's by a relative error of at most 0.005.
Values may be sent and summed in bfloat16 or wider, within the bound.
A program may use at most 64 MiB of HBM per device.

```python
import jax
import jax.numpy as jnp
from jax import lax

D = 8192
FF = 15360
TOKENS = 1024


def shard_levels(own_key, extent, cuts, smallest, top_value):
    def one(axis_at, parts):
        heights = jax.random.uniform(jax.random.fold_in(jax.random.fold_in(own_key, 6), axis_at), (parts,), jnp.float32, smallest / len(cuts), top_value / len(cuts))
        return jnp.repeat(jnp.exp(heights), extent[axis_at] // parts).reshape((-1,) + (1,) * (len(extent) - axis_at - 1))

    factor_of = one(*cuts[0])
    for cut in cuts[1:]:
        factor_of = factor_of * one(*cut)
    return factor_of


def centred(own_key, dims, spread, bound, pieces=(), held_as=jnp.bfloat16):
    gain = shard_levels(own_key, dims, pieces, -0.22, 0.18) if pieces else 1.0
    values = jax.random.normal(own_key, dims, jnp.float32) * spread * gain
    return jnp.minimum(jnp.maximum(values, -bound), bound).astype(held_as)


def setup_inputs(seed: int = 0) -> dict:
    seeds = jax.random.split(jax.random.key(seed), 6)
    tokens = centred(seeds[0], (TOKENS, D), 1.0, 6.0, ((0, 8), (1, 8)))
    cotangent = centred(seeds[1], (TOKENS, D), 1.0, 6.0, ((0, 8), (1, 8)))
    gate_weight = centred(seeds[2], (D, FF), D ** -0.5, 0.0625, ((0, 64), (1, 16)))
    up_weight = centred(seeds[3], (D, FF), D ** -0.5, 0.0625, ((0, 64), (1, 16)))
    down_weight = centred(seeds[4], (D, FF), FF ** -0.5, 0.046875, ((0, 64), (1, 16)))
    return {"tokens": tokens, "cotangent": cotangent, "gate_weight": gate_weight, "up_weight": up_weight, "down_weight": down_weight}


def reference(tokens, cotangent, gate_weight, up_weight, down_weight):
    gate = jnp.dot(tokens, gate_weight, preferred_element_type=jnp.float32)
    up = jnp.dot(tokens, up_weight, preferred_element_type=jnp.float32)
    sig = jax.nn.sigmoid(gate)
    hidden = (gate * sig * up).astype(jnp.bfloat16)
    contract = (((1,), (1,)), ((), ()))
    mixed = lax.dot_general(hidden, down_weight, contract, preferred_element_type=jnp.float32).astype(jnp.bfloat16)
    back = jnp.dot(cotangent, down_weight, preferred_element_type=jnp.float32)
    gate_grad = (back * up * sig * (1.0 + gate * (1.0 - sig))).astype(jnp.bfloat16)
    up_grad = (back * gate * sig).astype(jnp.bfloat16)
    total = lax.dot_general(gate_grad, gate_weight, contract, preferred_element_type=jnp.float32)
    total = total + lax.dot_general(up_grad, up_weight, contract, preferred_element_type=jnp.float32)
    return mixed, total.astype(jnp.bfloat16)
```

```python
import functools

import jax
import jax.numpy as jnp
from jax import lax
from jax.experimental import pallas as pl
from jax.experimental.pallas import tpu as pltpu
from jax.sharding import PartitionSpec as P

MESH = pl.DeviceIdType.MESH
CHUNKS = ((0, 256), (256, 256), (512, 256), (768, 192))
N = len(CHUNKS)
F32 = jnp.float32
BF16 = jnp.bfloat16
NT = (((1,), (1,)), ((), ()))


def kernel(*refs):
    refs = list(refs)

    def take(n):
        out = refs[:n]
        del refs[:n]
        return out

    tok, cot, gate_w, up_w, down_w = take(5)
    mixed_out, grad_out = take(2)
    (X,) = take(1)
    W, Pt, R, H = take(N), take(N), take(N), take(N)
    acc_m, acc_g, O, Q, O2, Z = take(6)
    x_send, x_recv = take(2)
    w_send, w_left, w_right, w_opp, w_pair = take(5)
    rs_send, rs_recv, ag_send, ag_recv = take(4)
    q_send, q_recv, z_send, z_recv = take(4)

    d = lax.axis_index("dp")
    t = lax.axis_index("tensor")
    s = lax.axis_index("section")
    yl, c = lax.div(t, 2), lax.rem(t, 2)
    x, h = lax.div(s, 2), lax.rem(s, 2)
    y = h * 4 + yl
    zh, zl = lax.div(d, 4), lax.rem(d, 4)

    pair = (d, 2 * yl + 1 - c, s)
    right = (d, t, lax.rem(x + 1, 4) * 2 + h)
    left = (d, t, lax.rem(x + 3, 4) * 2 + h)

    def along_y(q):
        return (d, 2 * lax.rem(q, 4) + c, x * 2 + lax.div(q, 4))

    def remote(src, dst, ss, rs, dev):
        return pltpu.make_async_remote_copy(
            src_ref=src, dst_ref=dst, send_sem=ss, recv_sem=rs, device_id=dev, device_id_type=MESH
        )

    def await_recv(ref, sem):
        remote(ref, ref, sem, sem, pair).wait_recv()

    def await_send(ref, sem):
        remote(ref, ref, sem, sem, pair).wait_send()

    own = pl.multiple_of(c * 512 + x * 128, 128)
    for f, (at, width) in enumerate(CHUNKS):
        for w, ref in enumerate((gate_w, up_w, down_w)):
            W[f][w, pl.ds(own, 128), :] = ref[:, at : at + width]

    barrier = pltpu.get_barrier_semaphore()
    partners = [pair, right, left, (d, 2 * yl + 1 - c, x * 2 + 1 - h)]
    partners += [along_y(lax.rem(y + k, 8)) for k in range(1, 8)]
    partners += [(zh * 4 + lax.rem(zl + k, 4), t, s) for k in range(1, 4)]
    for k in range(1, 4):
        far = lax.rem(zh + k, 4) * 4 + zl
        partners += [(far, 2 * yl + a, x * 2 + b) for a in range(2) for b in range(2)]
    for p in partners:
        pl.semaphore_signal(barrier, inc=1, device_id=p, device_id_type=MESH)
    pl.semaphore_wait(barrier, len(partners))

    def rows(core, at, size=128, extra=0):
        return pl.ds(pl.multiple_of(core * 512 + lax.rem(at, 4) * 128 + extra, 64), size)

    def start_own(f):
        mine = W[f].at[:, rows(c, x), :]
        remote(mine, mine, w_send.at[f], w_left.at[f], right).start()
        remote(mine, mine, w_send.at[f], w_right.at[f], left).start()
        remote(mine, mine, w_send.at[f], w_pair.at[f], pair).start()

    start_own(0)

    for a, ref in enumerate((tok, cot)):
        for other in range(2):
            to = lax.rem(h + other, 2)
            for b in range(4):
                src = ref.at[:, pl.ds(pl.multiple_of((b * 2 + to) * 128, 128), 128)]
                dst = X.at[a, :, pl.ds(pl.multiple_of(c * 512 + b * 128, 128), 128)]
                dev = (d, 2 * yl + h, x * 2 + to)
                if other:
                    remote(src, dst, x_send, x_recv, dev).start()
                else:

                    @pl.when(c == h)
                    def _():
                        pltpu.make_async_copy(src, dst, x_recv).start()

                    @pl.when(c != h)
                    def _():
                        remote(src, dst, x_send, x_recv, dev).start()

    start_own(1)
    acc_m[...] = jnp.zeros_like(acc_m)
    acc_g[...] = jnp.zeros_like(acc_g)

    def gather(f):
        fl = W[f].at[:, rows(c, x + 3), :]
        await_recv(fl, w_left.at[f])
        half = W[f].at[:, rows(c, x + 3, 64), :]
        remote(half, half, w_send.at[f], w_opp.at[f], right).start()
        remote(fl, fl, w_send.at[f], w_pair.at[f], pair).start()
        fr = W[f].at[:, rows(c, x + 1), :]
        await_recv(fr, w_right.at[f])
        half = W[f].at[:, rows(c, x + 1, 64, 64), :]
        remote(half, half, w_send.at[f], w_opp.at[f], left).start()
        remote(fr, fr, w_send.at[f], w_pair.at[f], pair).start()
        if f + 2 < N:
            start_own(f + 2)
        fo = W[f].at[:, rows(c, x + 2), :]
        await_recv(fo, w_opp.at[f])
        remote(fo, fo, w_send.at[f], w_pair.at[f], pair).start()
        await_recv(W[f].at[:, pl.ds(0, 512), :], w_pair.at[f])

    def partial_sums(f):
        width = CHUNKS[f][1]
        for w in range(3):
            part = jnp.dot(X[w // 2], W[f][w], preferred_element_type=F32)
            Pt[f][:, w, :, :] = part.astype(BF16).reshape(8, 16, width)
        for k in range(1, 8):
            q = lax.rem(y + k, 8)
            remote(
                Pt[f].at[q], R[f].at[k - 1], rs_send.at[f], rs_recv.at[f], along_y(q)
            ).start()

    def activate(f):
        await_recv(R[f], rs_recv.at[f])
        total = [Pt[f][y, w].astype(F32) for w in range(3)]
        for k in range(7):
            for w in range(3):
                total[w] = total[w] + R[f][k, w].astype(F32)
        gate, up, back = total
        sig = 1.0 / (1.0 + jnp.exp(-gate))
        H[f][y, 0] = (gate * sig * up).astype(BF16)
        H[f][y, 1] = (back * up * sig * (1.0 + gate * (1.0 - sig))).astype(BF16)
        H[f][y, 2] = (back * gate * sig).astype(BF16)
        for k in range(1, 8):
            mine = H[f].at[y]
            remote(
                mine, mine, ag_send.at[f], ag_recv.at[f], along_y(lax.rem(y + k, 8))
            ).start()

    def outputs(f):
        width = CHUNKS[f][1]
        await_recv(H[f].at[pl.ds(0, 7)], ag_recv.at[f])
        hid, gg, ug = (H[f][:, w].reshape(128, width) for w in range(3))
        acc_m[...] += lax.dot_general(hid, W[f][2], NT, preferred_element_type=F32)
        acc_g[...] += lax.dot_general(
            gg, W[f][0], NT, preferred_element_type=F32
        ) + lax.dot_general(ug, W[f][1], NT, preferred_element_type=F32)

    for step in range(N + 2):
        if step < N:
            gather(step)
            if step == 0:
                await_recv(X, x_recv)
            partial_sums(step)
        if 0 <= step - 1 < N:
            activate(step - 1)
        if 0 <= step - 2:
            outputs(step - 2)

    for e in range(16):
        for v in range(2):
            O[e % 4, e // 4, v, :, 0:512] = acc_m[
                e * 8 : e * 8 + 8, v * 512 : v * 512 + 512
            ].astype(BF16)
            O[e % 4, e // 4, v, :, 512:1024] = acc_g[
                e * 8 : e * 8 + 8, v * 512 : v * 512 + 512
            ].astype(BF16)
    for k in range(1, 4):
        to = lax.rem(zl + k, 4)
        remote(O.at[to], Q.at[k - 1], q_send, q_recv, (zh * 4 + to, t, s)).start()
    await_recv(Q, q_recv)
    for e in range(4):
        for v in range(2):
            part = O[zl, e, v].astype(F32)
            for k in range(3):
                part = part + Q[k, e, v].astype(F32)
            O2[e, v] = part.astype(BF16)
    for k in range(4):
        to = lax.rem(zh + k, 4)
        for v in range(2):
            src, dst = O2.at[to, v], Z.at[h * 4 + zh]
            dev = (to * 4 + zl, 2 * yl + v, x * 2 + c)
            if k:
                remote(src, dst, z_send, z_recv, dev).start()
            else:
                mine = jnp.logical_and(c == h, c == v)

                @pl.when(mine)
                def _():
                    pltpu.make_async_copy(src, dst, z_recv).start()

                @pl.when(jnp.logical_not(mine))
                def _():
                    remote(src, dst, z_send, z_recv, dev).start()

    await_recv(Z, z_recv)
    for b in range(2):
        total = Z[b * 4].astype(F32)
        for k in range(1, 4):
            total = total + Z[b * 4 + k].astype(F32)
        for a in range(4):
            to = (a * 2 + b) * 128
            mixed_out[:, to : to + 128] = total[:, a * 128 : a * 128 + 128].astype(BF16)
            grad_out[:, to : to + 128] = total[:, 512 + a * 128 : 640 + a * 128].astype(BF16)

    for f in range(N):
        await_send(W[f].at[:, pl.ds(0, 896), :], w_send.at[f])
        await_send(R[f], rs_send.at[f])
        await_send(H[f].at[pl.ds(0, 7)], ag_send.at[f])
    await_send(Q, q_send)

    @pl.when(c == h)
    def _():
        await_send(X.at[:, :, pl.ds(0, 512)], x_send)
        await_send(Z.at[pl.ds(0, 7)], z_send)

    @pl.when(c != h)
    def _():
        await_send(X, x_send)
        await_send(Z, z_send)


def body(*args):
    dma = pltpu.SemaphoreType.DMA
    widths = [w for _, w in CHUNKS]
    scratch = [pltpu.VMEM((2, 128, 1024), BF16)]
    scratch += [pltpu.VMEM((3, 1024, w), BF16) for w in widths]
    scratch += [pltpu.VMEM((8, 3, 16, w), BF16) for w in widths]
    scratch += [pltpu.VMEM((7, 3, 16, w), BF16) for w in widths]
    scratch += [pltpu.VMEM((8, 3, 16, w), BF16) for w in widths]
    scratch += [
        pltpu.VMEM((128, 1024), F32),
        pltpu.VMEM((128, 1024), F32),
        pltpu.VMEM((4, 4, 2, 8, 1024), BF16),
        pltpu.VMEM((3, 4, 2, 8, 1024), BF16),
        pltpu.VMEM((4, 2, 8, 1024), BF16),
        pltpu.VMEM((8, 8, 1024), BF16),
    ]
    scratch += [dma, dma]
    scratch += [dma((N,))] * 5
    scratch += [dma((N,))] * 4
    scratch += [dma] * 4
    vmem = pl.BlockSpec(memory_space=pltpu.VMEM)
    return pl.pallas_call(
        kernel,
        out_shape=[jax.ShapeDtypeStruct((8, 1024), BF16)] * 2,
        in_specs=[vmem] * 5,
        out_specs=[vmem] * 2,
        scratch_shapes=scratch,
        compiler_params=pltpu.CompilerParams(collective_id=0, has_side_effects=True),
        name="ffn",
    )(*args)


def solution(mesh):
    placed = (
        P("section", "tensor"),
        P("section", "tensor"),
        P(("tensor", "section"), "dp"),
        P(("tensor", "section"), "dp"),
        P(("tensor", "section"), "dp"),
    )
    return jax.shard_map(
        lambda *args: tuple(body(*args)),
        mesh=mesh,
        in_specs=placed,
        out_specs=(P(("section", "dp"), "tensor"), P(("section", "dp"), "tensor")),
        check_vma=False,
    )
```

```python
import jax
import jax.numpy as jnp
from jax import lax
from jax.experimental import pallas as pl
from jax.experimental.pallas import tpu as pltpu
from jax.sharding import PartitionSpec as P

MESH = pl.DeviceIdType.MESH
CHUNKS = ((0, 256), (256, 256), (512, 256), (768, 192))
N = len(CHUNKS)
UNITS = [("gu", f) for f in range(N)] + [("dn", f) for f in range(N)]
M = len(UNITS)
GU = [UNITS.index(("gu", f)) for f in range(N)]
DN = [UNITS.index(("dn", f)) for f in range(N)]
HOW_MANY = [2 if kind == "gu" else 1 for kind, _ in UNITS]
GATHERED = [1 if kind == "gu" else 2 for kind, _ in UNITS]
WIDTH = [CHUNKS[f][1] for _, f in UNITS]
F32 = jnp.float32
BF16 = jnp.bfloat16
NT = (((1,), (1,)), ((), ()))


def kernel(*refs):
    refs = list(refs)

    def take(n):
        out = refs[:n]
        del refs[:n]
        return out

    tok, cot, gate_w, up_w, down_w = take(5)
    mixed_out, grad_out = take(2)
    T, X = take(2)
    W, Pt, Pf, R, H = take(M), take(M), take(M), take(M), take(M)
    G = take(N)
    acc_m, acc_g, O, Q, O2, Z = take(6)
    t_load, w_load = take(2)
    x_send, x_recv = take(2)
    w_send, w_left, w_right, w_opp, w_pair = take(5)
    rs_send, rs_recv, ag_send, ag_recv = take(4)
    q_send, q_recv, z_send, z_recv = take(4)

    d = lax.axis_index("dp")
    t = lax.axis_index("tensor")
    s = lax.axis_index("section")
    yl, c = lax.div(t, 2), lax.rem(t, 2)
    x, h = lax.div(s, 2), lax.rem(s, 2)
    y = h * 4 + yl
    zh, zl = lax.div(d, 4), lax.rem(d, 4)

    pair = (d, 2 * yl + 1 - c, s)
    right = (d, t, lax.rem(x + 1, 4) * 2 + h)
    left = (d, t, lax.rem(x + 3, 4) * 2 + h)

    def along_y(q):
        return (d, 2 * lax.rem(q, 4) + c, x * 2 + lax.div(q, 4))

    def remote(src, dst, ss, rs, dev):
        return pltpu.make_async_remote_copy(
            src_ref=src, dst_ref=dst, send_sem=ss, recv_sem=rs, device_id=dev, device_id_type=MESH
        )

    def await_recv(ref, sem):
        remote(ref, ref, sem, sem, pair).wait_recv()

    def await_send(ref, sem):
        remote(ref, ref, sem, sem, pair).wait_send()

    def block(at):
        return c * 4 + lax.rem(at, 4)

    def lanes(at):
        return pl.ds(pl.multiple_of(at, 128), 128)

    for u, (kind, f) in enumerate(UNITS):
        at, width = CHUNKS[f]
        for w, ref in enumerate((gate_w, up_w) if kind == "gu" else (down_w,)):
            pltpu.make_async_copy(
                ref.at[pl.ds(at, width), :], W[u].at[w, block(x)], w_load.at[u]
            ).start()
        if u == 0:
            for a, ref in enumerate((tok, cot)):
                pltpu.make_async_copy(ref, T.at[a], t_load).start()

    @pl.when(c == h)
    def _():
        for a, ref in enumerate((tok, cot)):
            for b in range(4):
                pltpu.make_async_copy(
                    ref.at[:, lanes((b * 2 + h) * 128)],
                    X.at[a, :, lanes(c * 512 + b * 128)],
                    x_recv,
                ).start()

    barrier = pltpu.get_barrier_semaphore()
    partners = [pair, right, left, (d, 2 * yl + 1 - c, x * 2 + 1 - h)]
    partners += [along_y(lax.rem(y + k, 8)) for k in range(1, 8)]
    partners += [(zh * 4 + lax.rem(zl + k, 4), t, s) for k in range(1, 4)]
    for k in range(1, 4):
        far = lax.rem(zh + k, 4) * 4 + zl
        partners += [(far, 2 * yl + a, x * 2 + b) for a in range(2) for b in range(2)]
    for p in partners:
        pl.semaphore_signal(barrier, inc=1, device_id=p, device_id_type=MESH)
    acc_m[...] = jnp.zeros_like(acc_m)
    acc_g[...] = jnp.zeros_like(acc_g)
    pl.semaphore_wait(barrier, len(partners))

    def start_own(u):
        mine = W[u].at[:, block(x)]
        pltpu.make_async_copy(mine, mine, w_load.at[u]).wait()
        remote(mine, mine, w_send.at[u], w_left.at[u], right).start()
        remote(mine, mine, w_send.at[u], w_right.at[u], left).start()
        remote(mine, mine, w_send.at[u], w_pair.at[u], pair).start()

    start_own(0)

    pltpu.make_async_copy(T, T, t_load).wait()
    for other in (1, 0):
        to = lax.rem(h + other, 2)
        dev = (d, 2 * yl + h, x * 2 + to)

        def spread():
            for a in range(2):
                for b in range(4):
                    remote(
                        T.at[a, :, lanes((b * 2 + to) * 128)],
                        X.at[a, :, lanes(c * 512 + b * 128)],
                        x_send,
                        x_recv,
                        dev,
                    ).start()

        if other:
            spread()
        else:
            pl.when(c != h)(spread)

    start_own(1)

    def take_neighbours(u):
        half = WIDTH[u] // 2
        got = W[u].at[:, block(x + 3)]
        await_recv(got, w_left.at[u])
        some = W[u].at[:, block(x + 3), pl.ds(0, half)]
        remote(some, some, w_send.at[u], w_opp.at[u], right).start()
        remote(got, got, w_send.at[u], w_pair.at[u], pair).start()
        got = W[u].at[:, block(x + 1)]
        await_recv(got, w_right.at[u])
        some = W[u].at[:, block(x + 1), pl.ds(half, half)]
        remote(some, some, w_send.at[u], w_opp.at[u], left).start()
        remote(got, got, w_send.at[u], w_pair.at[u], pair).start()
        for v in {2: (4, 5)}.get(u, (u + 2 if u < 2 else u + 3,)):
            if v < M:
                start_own(v)

    def take_opposite(u):
        got = W[u].at[:, block(x + 2)]
        await_recv(got, w_opp.at[u])
        remote(got, got, w_send.at[u], w_pair.at[u], pair).start()
        await_recv(W[u].at[:, pl.ds(0, 4)], w_pair.at[u])

    def weight(u, w):
        return jnp.concatenate([W[u][w, b] for b in range(8)], axis=1)

    def partial_sums(u):
        kind, width = UNITS[u][0], WIDTH[u]
        rows = X[0 if kind == "gu" else 1]
        for w in range(HOW_MANY[u]):
            part = lax.dot_general(rows, weight(u, w), NT, preferred_element_type=F32)
            Pf[u][:, w] = part.reshape(8, 16, width)
            Pt[u][:, w] = part.astype(BF16).reshape(8, 16, width)
        for k in (4, 3, 5, 2, 6, 1, 7):
            q = lax.rem(y + k, 8)
            remote(
                Pt[u].at[q], R[u].at[k - 1], rs_send.at[u], rs_recv.at[u], along_y(q)
            ).start()

    def activate(u):
        kind, f = UNITS[u]
        await_recv(R[u], rs_recv.at[u])
        total = [Pf[u][y, w] for w in range(HOW_MANY[u])]
        for k in range(7):
            for w in range(HOW_MANY[u]):
                total[w] = total[w] + R[u][k, w].astype(F32)
        if kind == "gu":
            gate, up = total
            G[f][0], G[f][1] = gate, up
            sig = 1.0 / (1.0 + jnp.exp(-gate))
            H[u][y, 0] = (gate * sig * up).astype(BF16)
        else:
            (back,) = total
            gate, up = G[f][0], G[f][1]
            sig = 1.0 / (1.0 + jnp.exp(-gate))
            H[u][y, 0] = (back * up * sig * (1.0 + gate * (1.0 - sig))).astype(BF16)
            H[u][y, 1] = (back * gate * sig).astype(BF16)
        mine = H[u].at[y]
        for k in (4, 3, 5, 2, 6, 1, 7):
            remote(
                mine, mine, ag_send.at[u], ag_recv.at[u], along_y(lax.rem(y + k, 8))
            ).start()

    def mix(f):
        u = GU[f]
        await_recv(H[u].at[pl.ds(0, 7)], ag_recv.at[u])
        hid = H[u][:, 0].reshape(128, WIDTH[u])
        acc_m[...] += jnp.dot(hid, weight(DN[f], 0), preferred_element_type=F32)

    def grads(f):
        u = DN[f]
        await_recv(H[u].at[pl.ds(0, 7)], ag_recv.at[u])
        gg, ug = (H[u][:, w].reshape(128, WIDTH[u]) for w in range(2))
        acc_g[...] += jnp.dot(gg, weight(GU[f], 0), preferred_element_type=F32) + jnp.dot(
            ug, weight(GU[f], 1), preferred_element_type=F32
        )

    accs, outs = (acc_m, acc_g), (mixed_out, grad_out)

    def near_start(a):
        for e in range(16):
            for v in range(2):
                O[a, e % 4, e // 4, v] = accs[a][
                    e * 8 : e * 8 + 8, v * 512 : v * 512 + 512
                ].astype(BF16)
        for k in (3, 2, 1):
            to = lax.rem(zl + k, 4)
            remote(
                O.at[a, to], Q.at[a, k - 1], q_send.at[a], q_recv.at[a], (zh * 4 + to, t, s)
            ).start()

    def far_start(a):
        await_recv(Q.at[a], q_recv.at[a])
        for e in range(4):
            for v in range(2):
                part = accs[a][
                    pl.ds(pl.multiple_of(e * 32 + zl * 8, 8), 8), v * 512 : v * 512 + 512
                ]
                for k in range(3):
                    part = part + Q[a, k, e, v].astype(F32)
                O2[a, e, v] = part.astype(BF16)
        for k in (2, 1, 3, 0):
            to = lax.rem(zh + k, 4)
            for v in range(2):
                src, dst = O2.at[a, to, v], Z.at[a, h * 4 + zh]
                dev = (to * 4 + zl, 2 * yl + v, x * 2 + c)
                if k:
                    remote(src, dst, z_send.at[a], z_recv.at[a], dev).start()
                else:
                    mine = jnp.logical_and(c == h, c == v)

                    @pl.when(mine)
                    def _():
                        pltpu.make_async_copy(src, dst, z_recv.at[a]).start()

                    @pl.when(jnp.logical_not(mine))
                    def _():
                        remote(src, dst, z_send.at[a], z_recv.at[a], dev).start()

    def finish(a):
        await_recv(Z.at[a], z_recv.at[a])
        for b in range(2):
            total = Z[a, b * 4].astype(F32)
            for k in range(1, 4):
                total = total + Z[a, b * 4 + k].astype(F32)
            for e in range(4):
                to = (e * 2 + b) * 128
                outs[a][:, to : to + 128] = total[:, e * 128 : e * 128 + 128].astype(BF16)

    take_neighbours(0)
    for i in range(M + 2):
        if i + 1 < M:
            take_neighbours(i + 1)
        if i < M:
            take_opposite(i)
            if i == 0:
                await_recv(X, x_recv)
            partial_sums(i)
        if i >= 2:
            activate(i - 2)
        if i < M and UNITS[i][0] == "dn":
            mix(UNITS[i][1])
            if i == M - 1:
                near_start(0)
        if i >= 4 and UNITS[i - 4][0] == "dn":
            grads(UNITS[i - 4][1])
    far_start(0)
    grads(UNITS[M - 2][1])
    grads(UNITS[M - 1][1])
    near_start(1)
    far_start(1)
    finish(0)
    finish(1)

    for u in range(M):
        await_send(W[u].at[:, pl.ds(0, 7)], w_send.at[u])
        await_send(R[u], rs_send.at[u])
        await_send(H[u].at[pl.ds(0, 7)], ag_send.at[u])
    for a in range(2):
        await_send(Q.at[a], q_send.at[a])

    @pl.when(c == h)
    def _():
        await_send(X.at[:, :, pl.ds(0, 512)], x_send)
        for a in range(2):
            await_send(Z.at[a, pl.ds(0, 7)], z_send.at[a])

    @pl.when(c != h)
    def _():
        await_send(X, x_send)
        for a in range(2):
            await_send(Z.at[a], z_send.at[a])


def body(tokens, cotangent, gate_weight, up_weight, down_weight):
    dma = pltpu.SemaphoreType.DMA
    vmem = pltpu.VMEM
    scratch = [vmem((2, 128, 1024), BF16)] * 2
    units = list(zip(HOW_MANY, GATHERED, WIDTH))
    scratch += [vmem((n, 8, w, 128), BF16) for n, _, w in units]
    scratch += [vmem((8, n, 16, w), BF16) for n, _, w in units]
    scratch += [vmem((8, n, 16, w), F32) for n, _, w in units]
    scratch += [vmem((7, n, 16, w), BF16) for n, _, w in units]
    scratch += [vmem((8, n, 16, w), BF16) for _, n, w in units]
    scratch += [vmem((2, 16, w), F32) for _, w in CHUNKS]
    scratch += [
        vmem((128, 1024), F32),
        vmem((128, 1024), F32),
        vmem((2, 4, 4, 2, 8, 512), BF16),
        vmem((2, 3, 4, 2, 8, 512), BF16),
        vmem((2, 4, 2, 8, 512), BF16),
        vmem((2, 8, 8, 512), BF16),
    ]
    scratch += [dma, dma((M,)), dma, dma]
    scratch += [dma((M,))] * 5
    scratch += [dma((M,))] * 4
    scratch += [dma((2,))] * 4
    return pl.pallas_call(
        kernel,
        out_shape=[jax.ShapeDtypeStruct((8, 1024), BF16)] * 2,
        in_specs=[pl.BlockSpec(memory_space=pl.ANY)] * 5,
        out_specs=[pl.BlockSpec(memory_space=pltpu.VMEM)] * 2,
        scratch_shapes=scratch,
        compiler_params=pltpu.CompilerParams(collective_id=0, has_side_effects=True),
        name="ffn",
    )(tokens, cotangent, gate_weight.T, up_weight.T, down_weight.T)


def solution(mesh):
    placed = (
        P("section", "tensor"),
        P("section", "tensor"),
        P(("tensor", "section"), "dp"),
        P(("tensor", "section"), "dp"),
        P(("tensor", "section"), "dp"),
    )
    return jax.shard_map(
        lambda *args: tuple(body(*args)),
        mesh=mesh,
        in_specs=placed,
        out_specs=(P(("section", "dp"), "tensor"), P(("section", "dp"), "tensor")),
        check_vma=False,
    )
```

```python
import jax
import jax.numpy as jnp
from jax import lax
from jax.experimental import pallas as pl
from jax.experimental.pallas import tpu as pltpu
from jax.sharding import PartitionSpec as P

MESH = pl.DeviceIdType.MESH
CHUNKS = ((0, 192), (192, 256), (448, 256), (704, 256))
N = len(CHUNKS)
UNITS = [("gu", f) for f in range(N)] + [("dn", f) for f in range(N)]
M = len(UNITS)
GU = [UNITS.index(("gu", f)) for f in range(N)]
DN = [UNITS.index(("dn", f)) for f in range(N)]
HOW_MANY = [2 if kind == "gu" else 1 for kind, _ in UNITS]
GATHERED = [1 if kind == "gu" else 2 for kind, _ in UNITS]
WIDTH = [CHUNKS[f][1] for _, f in UNITS]
F32 = jnp.float32
BF16 = jnp.bfloat16
NT = (((1,), (1,)), ((), ()))
REACH = (1, 2, 4, 1)
FAR_FIRST = (8, 7, 9, 6, 10, 5, 11, 4, 12, 3, 13, 2, 14, 1, 15, 0)


def kernel(*refs):
    refs = list(refs)

    def take(n):
        out = refs[:n]
        del refs[:n]
        return out

    tok, cot, gate_w, up_w, down_w = take(5)
    mixed_out, grad_out = take(2)
    T, X = take(2)
    W, Pt, Pf, R, H = take(M), take(M), take(M), take(M), take(M)
    G = take(N)
    acc_m, acc_g, O, Z = take(4)
    t_load, w_load = take(2)
    x_send, x_recv = take(2)
    w_send, w_left, w_right, w_opp, w_pair = take(5)
    rs_send, rs_recv, ag_send, ag_recv, ag_low, ag_high = take(6)
    z_send, z_recv, ready = take(3)

    d = lax.axis_index("dp")
    t = lax.axis_index("tensor")
    s = lax.axis_index("section")
    yl, c = lax.div(t, 2), lax.rem(t, 2)
    x, h = lax.div(s, 2), lax.rem(s, 2)
    y = h * 4 + yl

    pair = (d, 2 * yl + 1 - c, s)
    right = (d, t, lax.rem(x + 1, 4) * 2 + h)
    left = (d, t, lax.rem(x + 3, 4) * 2 + h)

    def along_y(q):
        return (d, 2 * lax.rem(q, 4) + c, x * 2 + lax.div(q, 4))

    def remote(src, dst, ss, rs, dev):
        return pltpu.make_async_remote_copy(
            src_ref=src, dst_ref=dst, send_sem=ss, recv_sem=rs, device_id=dev, device_id_type=MESH
        )

    def await_recv(ref, sem):
        remote(ref, ref, sem, sem, pair).wait_recv()

    def await_send(ref, sem):
        remote(ref, ref, sem, sem, pair).wait_send()

    def block(at):
        return c * 4 + lax.rem(at, 4)

    def lanes(at):
        return pl.ds(pl.multiple_of(at, 128), 128)

    for u, (kind, f) in enumerate(UNITS):
        at, width = CHUNKS[f]
        for w, ref in enumerate((gate_w, up_w) if kind == "gu" else (down_w,)):
            pltpu.make_async_copy(
                ref.at[pl.ds(at, width), :], W[u].at[w, block(x)], w_load.at[u]
            ).start()
        if u == 0:
            for a, ref in enumerate((tok, cot)):
                pltpu.make_async_copy(ref, T.at[a], t_load).start()

    @pl.when(c == h)
    def _():
        for a, ref in enumerate((tok, cot)):
            for b in range(4):
                pltpu.make_async_copy(
                    ref.at[:, lanes((b * 2 + h) * 128)],
                    X.at[a, :, lanes(c * 512 + b * 128)],
                    x_recv.at[a],
                ).start()

    barrier = pltpu.get_barrier_semaphore()
    partners = [along_y(lax.rem(y + k, 8)) for k in (4, 3, 5, 2, 6, 1, 7)]
    partners += [(d, 2 * yl + 1 - c, x * 2 + 1 - h), right, left, pair]
    partners += [(lax.rem(d + k, 16), t, s) for k in (1, 15)]
    for p in partners:
        pl.semaphore_signal(barrier, inc=1, device_id=p, device_id_type=MESH)
    acc_m[...] = jnp.zeros_like(acc_m)
    acc_g[...] = jnp.zeros_like(acc_g)
    pl.semaphore_wait(barrier, len(partners))

    def tell(r):
        for k in (REACH[r], 16 - REACH[r]):
            pl.semaphore_signal(
                ready.at[r], inc=1, device_id=(lax.rem(d + k, 16), t, s), device_id_type=MESH
            )

    tell(0)

    def start_own(u):
        mine = W[u].at[:, block(x)]
        pltpu.make_async_copy(mine, mine, w_load.at[u]).wait()
        remote(mine, mine, w_send.at[u], w_left.at[u], right).start()
        remote(mine, mine, w_send.at[u], w_right.at[u], left).start()
        remote(mine, mine, w_send.at[u], w_pair.at[u], pair).start()

    start_own(0)

    pltpu.make_async_copy(T, T, t_load).wait()
    for a in range(2):
        for other in (1, 0):
            to = lax.rem(h + other, 2)
            dev = (d, 2 * yl + h, x * 2 + to)

            def spread():
                for b in range(4):
                    remote(
                        T.at[a, :, lanes((b * 2 + to) * 128)],
                        X.at[a, :, lanes(c * 512 + b * 128)],
                        x_send,
                        x_recv.at[a],
                        dev,
                    ).start()

            if other:
                spread()
            else:
                pl.when(c != h)(spread)

    start_own(1)

    def take_neighbours(u):
        half = WIDTH[u] // 2
        got = W[u].at[:, block(x + 3)]
        await_recv(got, w_left.at[u])
        some = W[u].at[:, block(x + 3), pl.ds(0, half)]
        remote(some, some, w_send.at[u], w_opp.at[u], right).start()
        remote(got, got, w_send.at[u], w_pair.at[u], pair).start()
        got = W[u].at[:, block(x + 1)]
        await_recv(got, w_right.at[u])
        some = W[u].at[:, block(x + 1), pl.ds(half, half)]
        remote(some, some, w_send.at[u], w_opp.at[u], left).start()
        remote(got, got, w_send.at[u], w_pair.at[u], pair).start()
        for v in {2: (4, 5)}.get(u, (u + 2 if u < 2 else u + 3,)):
            if v < M:
                start_own(v)

    def take_opposite(u):
        got = W[u].at[:, block(x + 2)]
        await_recv(got, w_opp.at[u])
        remote(got, got, w_send.at[u], w_pair.at[u], pair).start()
        await_recv(W[u].at[:, pl.ds(0, 4)], w_pair.at[u])

    def weight(u, w):
        return jnp.concatenate([W[u][w, b] for b in range(8)], axis=1)

    def partial_sums(u):
        kind, width = UNITS[u][0], WIDTH[u]
        rows = X[0 if kind == "gu" else 1]
        for w in range(HOW_MANY[u]):
            part = lax.dot_general(rows, weight(u, w), NT, preferred_element_type=F32)
            Pf[u][:, w] = part.reshape(8, 16, width)
            Pt[u][:, w] = part.astype(BF16).reshape(8, 16, width)
        for k in (4, 3, 5, 2, 6, 1, 7):
            q = lax.rem(y + k, 8)
            remote(
                Pt[u].at[q], R[u].at[k - 1], rs_send.at[u], rs_recv.at[u], along_y(q)
            ).start()

    def activate(u):
        kind, f = UNITS[u]
        await_recv(R[u], rs_recv.at[u])
        total = [Pf[u][y, w] for w in range(HOW_MANY[u])]
        for k in range(7):
            for w in range(HOW_MANY[u]):
                total[w] = total[w] + R[u][k, w].astype(F32)
        if kind == "gu":
            gate, up = total
            G[f][0], G[f][1] = gate, up
            sig = 1.0 / (1.0 + jnp.exp(-gate))
            H[u][y, 0] = (gate * sig * up).astype(BF16)
        else:
            (back,) = total
            gate, up = G[f][0], G[f][1]
            sig = 1.0 / (1.0 + jnp.exp(-gate))
            H[u][y, 0] = (back * up * sig * (1.0 + gate * (1.0 - sig))).astype(BF16)
            H[u][y, 1] = (back * gate * sig).astype(BF16)
        mine = H[u].at[y]
        for k, sem in ((2, ag_low), (6, ag_high), (1, ag_recv), (7, ag_recv)):
            remote(
                mine, mine, ag_send.at[u], sem.at[u], along_y(lax.rem(y + k, 8))
            ).start()

    def halves(u, src):
        if GATHERED[u] == 2:
            return H[u].at[src, 0], H[u].at[src, 1]
        if WIDTH[u] == 256:
            return H[u].at[src, :, :, pl.ds(0, 128)], H[u].at[src, :, :, pl.ds(128, 128)]
        return H[u].at[src], None

    def relay(u):
        for side, sem in ((0, ag_low), (1, ag_high)):
            src = lax.rem(y + (6, 2)[side], 8)
            got, part = H[u].at[src], halves(u, src)[side]
            await_recv(got, sem.at[u])
            if part is not None:
                to = along_y(lax.rem(y + (2, 6)[side], 8))
                remote(part, part, ag_send.at[u], ag_recv.at[u], to).start()
            to = along_y(lax.rem(y + (1, 7)[side], 8))
            remote(got, got, ag_send.at[u], ag_recv.at[u], to).start()

    def mix(f):
        u = GU[f]
        await_recv(H[u].at[pl.ds(0, 5)], ag_recv.at[u])
        hid = H[u][:, 0].reshape(128, WIDTH[u])
        acc_m[...] += jnp.dot(hid, weight(DN[f], 0), preferred_element_type=F32)

    def grads(f):
        u = DN[f]
        await_recv(H[u].at[pl.ds(0, 5)], ag_recv.at[u])
        gg, ug = (H[u][:, w].reshape(128, WIDTH[u]) for w in range(2))
        acc_g[...] += jnp.dot(gg, weight(GU[f], 0), preferred_element_type=F32) + jnp.dot(
            ug, weight(GU[f], 1), preferred_element_type=F32
        )

    accs, outs = (acc_m, acc_g), (mixed_out, grad_out)

    def scatter(a):
        for e in range(16):
            for v in range(2):
                O[a, e, v] = accs[a][e * 8 : e * 8 + 8, v * 512 : v * 512 + 512].astype(BF16)
        for k in FAR_FIRST:
            to = lax.rem(d + k, 16)
            for v in range(2):
                src, dst = O.at[a, to, v], Z.at[a, h * 16 + d]
                dev = (to, 2 * yl + v, x * 2 + c)
                if k:
                    remote(src, dst, z_send.at[a], z_recv.at[a], dev).start()
                else:
                    mine = jnp.logical_and(c == h, c == v)

                    @pl.when(mine)
                    def _():
                        pltpu.make_async_copy(src, dst, z_recv.at[a]).start()

                    @pl.when(jnp.logical_not(mine))
                    def _():
                        remote(src, dst, z_send.at[a], z_recv.at[a], dev).start()

    def finish(a):
        await_recv(Z.at[a], z_recv.at[a])
        for b in range(2):
            total = Z[a, b * 16].astype(F32)
            for k in range(1, 16):
                total = total + Z[a, b * 16 + k].astype(F32)
            for e in range(4):
                to = (e * 2 + b) * 128
                outs[a][:, to : to + 128] = total[:, e * 128 : e * 128 + 128].astype(BF16)

    take_neighbours(0)
    for i in range(M + 2):
        if i + 1 < M:
            take_neighbours(i + 1)
        if i < M:
            take_opposite(i)
            if i == 0:
                await_recv(X.at[0], x_recv.at[0])
            if i == DN[0]:
                await_recv(X.at[1], x_recv.at[1])
            partial_sums(i)
            if i < len(REACH):
                pl.semaphore_wait(ready.at[i], 2)
                if i + 1 < len(REACH):
                    tell(i + 1)
        if i >= 2:
            activate(i - 2)
        if i >= 3:
            relay(i - 3)
        if i < M and UNITS[i][0] == "dn":
            mix(UNITS[i][1])
            if i == M - 1:
                scatter(0)
        if i >= 4 and UNITS[i - 4][0] == "dn":
            grads(UNITS[i - 4][1])
    relay(M - 1)
    grads(UNITS[M - 2][1])
    grads(UNITS[M - 1][1])
    scatter(1)
    finish(0)
    finish(1)

    for u in range(M):
        await_send(W[u].at[:, pl.ds(0, 7)], w_send.at[u])
        await_send(R[u], rs_send.at[u])
        await_send(H[u].at[pl.ds(0, 7)], ag_send.at[u])
    @pl.when(c == h)
    def _():
        await_send(X.at[:, :, pl.ds(0, 512)], x_send)
        for a in range(2):
            await_send(Z.at[a, pl.ds(0, 31)], z_send.at[a])

    @pl.when(c != h)
    def _():
        await_send(X, x_send)
        for a in range(2):
            await_send(Z.at[a], z_send.at[a])


def body(tokens, cotangent, gate_weight, up_weight, down_weight):
    dma = pltpu.SemaphoreType.DMA
    vmem = pltpu.VMEM
    scratch = [vmem((2, 128, 1024), BF16)] * 2
    units = list(zip(HOW_MANY, GATHERED, WIDTH))
    scratch += [vmem((n, 8, w, 128), BF16) for n, _, w in units]
    scratch += [vmem((8, n, 16, w), BF16) for n, _, w in units]
    scratch += [vmem((8, n, 16, w), F32) for n, _, w in units]
    scratch += [vmem((7, n, 16, w), BF16) for n, _, w in units]
    scratch += [vmem((8, n, 16, w), BF16) for _, n, w in units]
    scratch += [vmem((2, 16, w), F32) for _, w in CHUNKS]
    scratch += [
        vmem((128, 1024), F32),
        vmem((128, 1024), F32),
        vmem((2, 16, 2, 8, 512), BF16),
        vmem((2, 32, 8, 512), BF16),
    ]
    scratch += [dma, dma((M,)), dma, dma((2,))]
    scratch += [dma((M,))] * 5
    scratch += [dma((M,))] * 6
    scratch += [dma((2,))] * 2 + [pltpu.SemaphoreType.REGULAR((len(REACH),))]
    return pl.pallas_call(
        kernel,
        out_shape=[jax.ShapeDtypeStruct((8, 1024), BF16)] * 2,
        in_specs=[pl.BlockSpec(memory_space=pl.ANY)] * 5,
        out_specs=[pl.BlockSpec(memory_space=pltpu.VMEM)] * 2,
        scratch_shapes=scratch,
        compiler_params=pltpu.CompilerParams(collective_id=0, has_side_effects=True),
        name="ffn",
    )(tokens, cotangent, gate_weight.T, up_weight.T, down_weight.T)


def solution(mesh):
    placed = (
        P("section", "tensor"),
        P("section", "tensor"),
        P(("tensor", "section"), "dp"),
        P(("tensor", "section"), "dp"),
        P(("tensor", "section"), "dp"),
    )
    return jax.shard_map(
        lambda *args: tuple(body(*args)),
        mesh=mesh,
        in_specs=placed,
        out_specs=(P(("section", "dp"), "tensor"), P(("section", "dp"), "tensor")),
        check_vma=False,
    )
```

```python
import jax
import jax.numpy as jnp
from jax import lax
from jax.experimental import pallas as pl
from jax.experimental.pallas import tpu as pltpu
from jax.sharding import PartitionSpec as P

MESH = pl.DeviceIdType.MESH
CHUNKS = ((0, 192), (192, 256), (448, 256), (704, 256))
N = len(CHUNKS)
UNITS = [("gu", f) for f in range(N)] + [("dn", f) for f in range(N)]
M = len(UNITS)
GU = [UNITS.index(("gu", f)) for f in range(N)]
DN = [UNITS.index(("dn", f)) for f in range(N)]
HOW_MANY = [2 if kind == "gu" else 1 for kind, _ in UNITS]
GATHERED = [1 if kind == "gu" else 2 for kind, _ in UNITS]
WIDTH = [CHUNKS[f][1] for _, f in UNITS]
F32 = jnp.float32
BF16 = jnp.bfloat16
NT = (((1,), (1,)), ((), ()))
REACH = (1, 2, 4, 1)
FAR_FIRST = (8, 7, 9, 6, 10, 5, 11, 4, 12, 3, 13, 2, 14, 1, 15, 0)


def kernel(*refs):
    refs = list(refs)

    def take(n):
        out = refs[:n]
        del refs[:n]
        return out

    tok, cot, gate_w, up_w, down_w = take(5)
    (out,) = take(1)
    T, X = take(2)
    W, Pt, Pf, R, H = take(M), take(M), take(M), take(M), take(M)
    G = take(N)
    acc_m, acc_g, O, Z = take(4)
    t_load, w_load = take(2)
    x_send, x_recv = take(2)
    w_send, w_left, w_right, w_opp, w_pair = take(5)
    rs_send, rs_recv, ag_send, ag_recv, ag_low, ag_high = take(6)
    z_send, z_recv, ready = take(3)

    d = lax.axis_index("dp")
    t = lax.axis_index("tensor")
    s = lax.axis_index("section")
    yl, c = lax.div(t, 2), lax.rem(t, 2)
    x, h = lax.div(s, 2), lax.rem(s, 2)
    y = h * 4 + yl

    pair = (d, 2 * yl + 1 - c, s)
    right = (d, t, lax.rem(x + 1, 4) * 2 + h)
    left = (d, t, lax.rem(x + 3, 4) * 2 + h)

    def along_y(q):
        return (d, 2 * lax.rem(q, 4) + c, x * 2 + lax.div(q, 4))

    def remote(src, dst, ss, rs, dev):
        return pltpu.make_async_remote_copy(
            src_ref=src, dst_ref=dst, send_sem=ss, recv_sem=rs, device_id=dev, device_id_type=MESH
        )

    def await_recv(ref, sem):
        remote(ref, ref, sem, sem, pair).wait_recv()

    def await_send(ref, sem):
        remote(ref, ref, sem, sem, pair).wait_send()

    def block(at):
        return c * 4 + lax.rem(at, 4)

    def lanes(at):
        return pl.ds(pl.multiple_of(at, 128), 128)

    for u, (kind, f) in enumerate(UNITS):
        at, width = CHUNKS[f]
        for w, ref in enumerate((gate_w, up_w) if kind == "gu" else (down_w,)):
            pltpu.make_async_copy(
                ref.at[pl.ds(at, width), :], W[u].at[w, block(x)], w_load.at[u]
            ).start()
        if u == 0:
            for a, ref in enumerate((tok, cot)):
                pltpu.make_async_copy(ref, T.at[a], t_load).start()

    @pl.when(c == h)
    def _():
        for a, ref in enumerate((tok, cot)):
            for b in range(4):
                pltpu.make_async_copy(
                    ref.at[:, lanes((b * 2 + h) * 128)],
                    X.at[a, :, lanes(c * 512 + b * 128)],
                    x_recv.at[a],
                ).start()

    barrier = pltpu.get_barrier_semaphore()
    partners = [along_y(lax.rem(y + k, 8)) for k in (4, 3, 5, 2, 6, 1, 7)]
    partners += [(d, 2 * yl + 1 - c, x * 2 + 1 - h), right, left, pair]
    partners += [(lax.rem(d + k, 16), t, s) for k in (1, 15)]
    for p in partners:
        pl.semaphore_signal(barrier, inc=1, device_id=p, device_id_type=MESH)
    acc_m[...] = jnp.zeros_like(acc_m)
    acc_g[...] = jnp.zeros_like(acc_g)
    pl.semaphore_wait(barrier, len(partners))

    def tell(r):
        for k in (REACH[r], 16 - REACH[r]):
            pl.semaphore_signal(
                ready.at[r], inc=1, device_id=(lax.rem(d + k, 16), t, s), device_id_type=MESH
            )

    tell(0)

    def start_own(u):
        mine = W[u].at[:, block(x)]
        pltpu.make_async_copy(mine, mine, w_load.at[u]).wait()
        remote(mine, mine, w_send.at[u], w_left.at[u], right).start()
        remote(mine, mine, w_send.at[u], w_right.at[u], left).start()
        remote(mine, mine, w_send.at[u], w_pair.at[u], pair).start()

    start_own(0)

    pltpu.make_async_copy(T, T, t_load).wait()
    for a in range(2):
        for other in (1, 0):
            to = lax.rem(h + other, 2)
            dev = (d, 2 * yl + h, x * 2 + to)

            def spread():
                for b in range(4):
                    remote(
                        T.at[a, :, lanes((b * 2 + to) * 128)],
                        X.at[a, :, lanes(c * 512 + b * 128)],
                        x_send,
                        x_recv.at[a],
                        dev,
                    ).start()

            if other:
                spread()
            else:
                pl.when(c != h)(spread)

    start_own(1)

    def take_neighbours(u):
        half = WIDTH[u] // 2
        got = W[u].at[:, block(x + 3)]
        await_recv(got, w_left.at[u])
        some = W[u].at[:, block(x + 3), pl.ds(0, half)]
        remote(some, some, w_send.at[u], w_opp.at[u], right).start()
        remote(got, got, w_send.at[u], w_pair.at[u], pair).start()
        got = W[u].at[:, block(x + 1)]
        await_recv(got, w_right.at[u])
        some = W[u].at[:, block(x + 1), pl.ds(half, half)]
        remote(some, some, w_send.at[u], w_opp.at[u], left).start()
        remote(got, got, w_send.at[u], w_pair.at[u], pair).start()
        for v in {2: (4, 5)}.get(u, (u + 2 if u < 2 else u + 3,)):
            if v < M:
                start_own(v)

    def take_opposite(u):
        got = W[u].at[:, block(x + 2)]
        await_recv(got, w_opp.at[u])
        remote(got, got, w_send.at[u], w_pair.at[u], pair).start()
        await_recv(W[u].at[:, pl.ds(0, 4)], w_pair.at[u])

    def weight(u, w):
        return jnp.concatenate([W[u][w, b] for b in range(8)], axis=1)

    def partial_sums(u):
        kind, width = UNITS[u][0], WIDTH[u]
        rows = X[0 if kind == "gu" else 1]
        for w in range(HOW_MANY[u]):
            part = lax.dot_general(rows, weight(u, w), NT, preferred_element_type=F32)
            Pf[u][:, w] = part.reshape(8, 16, width)
            Pt[u][:, w] = part.astype(BF16).reshape(8, 16, width)
        for k in (4, 3, 5, 2, 6, 1, 7):
            q = lax.rem(y + k, 8)
            remote(
                Pt[u].at[q], R[u].at[k - 1], rs_send.at[u], rs_recv.at[u], along_y(q)
            ).start()

    def activate(u):
        kind, f = UNITS[u]
        await_recv(R[u], rs_recv.at[u])
        total = [Pf[u][y, w] for w in range(HOW_MANY[u])]
        for k in range(7):
            for w in range(HOW_MANY[u]):
                total[w] = total[w] + R[u][k, w].astype(F32)
        if kind == "gu":
            gate, up = total
            G[f][0], G[f][1] = gate, up
            sig = 1.0 / (1.0 + jnp.exp(-gate))
            H[u][y, 0] = (gate * sig * up).astype(BF16)
        else:
            (back,) = total
            gate, up = G[f][0], G[f][1]
            sig = 1.0 / (1.0 + jnp.exp(-gate))
            H[u][y, 0] = (back * up * sig * (1.0 + gate * (1.0 - sig))).astype(BF16)
            H[u][y, 1] = (back * gate * sig).astype(BF16)
        mine = H[u].at[y]
        for k, sem in ((2, ag_low), (6, ag_high), (1, ag_recv), (7, ag_recv)):
            remote(
                mine, mine, ag_send.at[u], sem.at[u], along_y(lax.rem(y + k, 8))
            ).start()

    def halves(u, src):
        if GATHERED[u] == 2:
            return H[u].at[src, 0], H[u].at[src, 1]
        if WIDTH[u] == 256:
            return H[u].at[src, :, :, pl.ds(0, 128)], H[u].at[src, :, :, pl.ds(128, 128)]
        return H[u].at[src], None

    def relay(u):
        for side, sem in ((0, ag_low), (1, ag_high)):
            src = lax.rem(y + (6, 2)[side], 8)
            got, part = H[u].at[src], halves(u, src)[side]
            await_recv(got, sem.at[u])
            if part is not None:
                to = along_y(lax.rem(y + (2, 6)[side], 8))
                remote(part, part, ag_send.at[u], ag_recv.at[u], to).start()
            to = along_y(lax.rem(y + (1, 7)[side], 8))
            remote(got, got, ag_send.at[u], ag_recv.at[u], to).start()

    def mix(f):
        u = GU[f]
        await_recv(H[u].at[pl.ds(0, 5)], ag_recv.at[u])
        hid = H[u][:, 0].reshape(128, WIDTH[u])
        acc_m[...] += jnp.dot(hid, weight(DN[f], 0), preferred_element_type=F32)

    def grads(f):
        u = DN[f]
        await_recv(H[u].at[pl.ds(0, 5)], ag_recv.at[u])
        gg, ug = (H[u][:, w].reshape(128, WIDTH[u]) for w in range(2))
        acc_g[...] += jnp.dot(gg, weight(GU[f], 0), preferred_element_type=F32) + jnp.dot(
            ug, weight(GU[f], 1), preferred_element_type=F32
        )

    accs = (acc_m, acc_g)

    def scatter(a):
        for e in range(16):
            for v in range(2):
                O[a, e, v] = accs[a][e * 8 : e * 8 + 8, v * 512 : v * 512 + 512].astype(BF16)
        for k in FAR_FIRST:
            to = lax.rem(d + k, 16)
            for v in range(2):
                src, dst = O.at[a, to, v], Z.at[a, h * 16 + d]
                dev = (to, 2 * yl + v, x * 2 + c)
                if k:
                    remote(src, dst, z_send.at[a], z_recv.at[a], dev).start()
                else:
                    mine = jnp.logical_and(c == h, c == v)

                    @pl.when(mine)
                    def _():
                        pltpu.make_async_copy(src, dst, z_recv.at[a]).start()

                    @pl.when(jnp.logical_not(mine))
                    def _():
                        remote(src, dst, z_send.at[a], z_recv.at[a], dev).start()

    def finish(a):
        await_recv(Z.at[a], z_recv.at[a])
        for b in range(2):
            total = Z[a, b * 16].astype(F32)
            for k in range(1, 16):
                total = total + Z[a, b * 16 + k].astype(F32)
            for e in range(4):
                to = (e * 2 + b) * 128
                out[a, :, to : to + 128] = total[:, e * 128 : e * 128 + 128].astype(BF16)

    take_neighbours(0)
    for i in range(M + 2):
        if i + 1 < M:
            take_neighbours(i + 1)
        if i < M:
            take_opposite(i)
            if i == 0:
                await_recv(X.at[0], x_recv.at[0])
            if i == DN[0]:
                await_recv(X.at[1], x_recv.at[1])
            partial_sums(i)
            if i < len(REACH):
                pl.semaphore_wait(ready.at[i], 2)
                if i + 1 < len(REACH):
                    tell(i + 1)
        if i >= 2:
            activate(i - 2)
        if i >= 3:
            relay(i - 3)
        if i < M and UNITS[i][0] == "dn":
            mix(UNITS[i][1])
            if i == M - 1:
                scatter(0)
        if i >= 4 and UNITS[i - 4][0] == "dn":
            grads(UNITS[i - 4][1])
    relay(M - 1)
    grads(UNITS[M - 2][1])
    grads(UNITS[M - 1][1])
    scatter(1)
    finish(0)
    finish(1)

    for u in range(M):
        await_send(W[u].at[:, pl.ds(0, 7)], w_send.at[u])
        await_send(R[u], rs_send.at[u])
        await_send(H[u].at[pl.ds(0, 7)], ag_send.at[u])
    @pl.when(c == h)
    def _():
        await_send(X.at[:, :, pl.ds(0, 512)], x_send)
        for a in range(2):
            await_send(Z.at[a, pl.ds(0, 31)], z_send.at[a])

    @pl.when(c != h)
    def _():
        await_send(X, x_send)
        for a in range(2):
            await_send(Z.at[a], z_send.at[a])


def body(tokens, cotangent, gate_weight, up_weight, down_weight):
    dma = pltpu.SemaphoreType.DMA
    vmem = pltpu.VMEM
    scratch = [vmem((2, 128, 1024), BF16)] * 2
    units = list(zip(HOW_MANY, GATHERED, WIDTH))
    scratch += [vmem((n, 8, w, 128), BF16) for n, _, w in units]
    scratch += [vmem((8, n, 16, w), BF16) for n, _, w in units]
    scratch += [vmem((8, n, 16, w), F32) for n, _, w in units]
    scratch += [vmem((7, n, 16, w), BF16) for n, _, w in units]
    scratch += [vmem((8, n, 16, w), BF16) for _, n, w in units]
    scratch += [vmem((2, 16, w), F32) for _, w in CHUNKS]
    scratch += [
        vmem((128, 1024), F32),
        vmem((128, 1024), F32),
        vmem((2, 16, 2, 8, 512), BF16),
        vmem((2, 32, 8, 512), BF16),
    ]
    scratch += [dma, dma((M,)), dma, dma((2,))]
    scratch += [dma((M,))] * 5
    scratch += [dma((M,))] * 6
    scratch += [dma((2,))] * 2 + [pltpu.SemaphoreType.REGULAR((len(REACH),))]
    both = pl.pallas_call(
        kernel,
        out_shape=jax.ShapeDtypeStruct((2, 8, 1024), BF16),
        in_specs=[pl.BlockSpec(memory_space=pl.ANY)] * 5,
        out_specs=pl.BlockSpec(memory_space=pltpu.VMEM),
        scratch_shapes=scratch,
        compiler_params=pltpu.CompilerParams(collective_id=0, has_side_effects=True),
        name="ffn",
    )(tokens, cotangent, gate_weight.T, up_weight.T, down_weight.T)
    return both[0], both[1]


def solution(mesh):
    placed = (
        P("section", "tensor"),
        P("section", "tensor"),
        P(("tensor", "section"), "dp"),
        P(("tensor", "section"), "dp"),
        P(("tensor", "section"), "dp"),
    )
    return jax.shard_map(
        lambda *args: tuple(body(*args)),
        mesh=mesh,
        in_specs=placed,
        out_specs=(P(("section", "dp"), "tensor"), P(("section", "dp"), "tensor")),
        check_vma=False,
    )
```
